32 devices in a mesh: dp: 4 (over y, x), row: 4 (over z), col: 2 (over core).
Axes of the slice: x: 2, y: 2, z: 4, core: 2. Of those that a mesh axis runs over, the one named last changes fastest.
Arguments:
- activations: bfloat16 [4, 64, 128, 512], P('dp', None, 'row', 'col'), may hold values from -18 to 18
- kernel: bfloat16 [3, 3, 64, 64], replicated, may hold values from -0.125 to 0.125
- gain: float32 [64], replicated, may hold values from 0.25 to 1.75
- cotangent: bfloat16 [4, 64, 128, 512], P('dp', None, 'row', 'col'), may hold values from -16 to 16
Outputs:
- input_grad: bfloat16 [4, 64, 128, 512], P('dp', None, 'row', 'col')
- weight_grad: float32 [3, 3, 64, 64], P(None, None, 'dp')
- gain_grad: float32 [64], replicated
- shift_grad: float32 [64], replicated
The draws below stay inside these ranges and needn't reach their ends.
All inputs are finite; a program needn't handle non-finite values.
Results may differ from the reference program's by a relative error of at most 0.0049.
Values may be sent and summed in bfloat16 or wider, within the bound.
A program may use at most 64 MiB of HBM per device.

```python
import jax
import jax.numpy as jnp
from jax import lax

C = 64
B = 4
H = 128
W = 512
PIXELS = 262144


def make_activations(key):
    noise_key = jax.random.fold_in(key, 11)
    offset_key = jax.random.fold_in(key, 23)
    heights = jnp.arange(H, dtype=jnp.float32) / max(H - 1, 1)
    offsets = jax.random.uniform(offset_key, (C,), jnp.float32, -0.2, 0.2)
    noise = jnp.clip(jax.random.normal(noise_key, (B, C, H, W), jnp.float32), -4.0, 4.0)
    scales = 1.0 + 2.0 * heights
    values = noise * scales[None, None, :, None] + offsets[None, :, None, None]
    return values.astype(jnp.bfloat16)


def make_kernel(key):
    kernel_key = jax.random.fold_in(key, 37)
    bound = 1.0 / C ** 0.5
    values = jnp.clip(jax.random.normal(kernel_key, (3, 3, C, C), jnp.float32) * (bound / 3.0), -bound, bound)
    return values.astype(jnp.bfloat16)


def draw_activations(key, part):
    return make_activations(key)


def draw_kernel(key, part):
    return make_kernel(key)


def signed_levels(key, low, high):
    sign_key = jax.random.fold_in(key, 1)
    size_key = jax.random.fold_in(key, 2)
    signs = jnp.where(jax.random.bernoulli(sign_key, 0.5, (C,)), 1.0, -1.0).astype(jnp.float32)
    return signs * jax.random.uniform(size_key, (C,), jnp.float32, low, high)


def draw_cotangent(key, part):
    images = make_activations(key)
    weights = make_kernel(key).astype(jnp.float32)
    offsets = signed_levels(jax.random.fold_in(key, 41), 0.2, 0.5)
    coupling = signed_levels(jax.random.fold_in(key, 43), 0.3, 1.0)
    noise_key = jax.random.fold_in(key, 47)
    heights = jnp.arange(H, dtype=jnp.float32) / max(H - 1, 1)
    span = float(max(B - 1, 1))

    def one_image(pair):
        image, index = pair
        place = index.astype(jnp.float32) / span
        pre = lax.conv_general_dilated(image.astype(jnp.float32)[None], weights, (1, 1), ((1, 1), (1, 1)), dimension_numbers=('NCHW', 'HWOI', 'NCHW'), precision=lax.Precision.HIGHEST)[0]
        centre = jnp.mean(pre, axis=(1, 2))
        spread = jnp.mean((pre - centre[:, None, None]) ** 2, axis=(1, 2))
        normed = jnp.clip((pre - centre[:, None, None]) * lax.rsqrt(spread + 1e-05)[:, None, None], -6.0, 6.0)
        image_key = jax.random.fold_in(noise_key, index)
        noise = jnp.clip(jax.random.normal(image_key, (C, H, W), jnp.float32), -4.0, 4.0)
        ramp = 0.5 + 0.5 * (place + heights)
        image_ramp = 0.5 + place
        values = noise + offsets[:, None, None] * ramp[None, :, None] + (coupling * image_ramp)[:, None, None] * normed
        return values.astype(jnp.bfloat16)
    return lax.map(one_image, (images, jnp.arange(B, dtype=jnp.int32)))


def setup_inputs(seed: int = 0) -> dict:
    seeds = jax.random.split(jax.random.key(seed), 5)
    return {
        "activations": draw_activations(jax.random.fold_in(seeds[4], 71), 0),
        "kernel": draw_kernel(jax.random.fold_in(seeds[4], 71), 0),
        "gain": jnp.clip(1.0 + 0.15 * jax.random.normal(seeds[2], (C,), jnp.float32), 0.25, 1.75),
        "cotangent": draw_cotangent(jax.random.fold_in(seeds[4], 71), 0),
    }


def convolve(image, weights):
    return lax.conv_general_dilated(image[None], weights, (1, 1), ((1, 1), (1, 1)), dimension_numbers=('NCHW', 'HWOI', 'NCHW'), precision=lax.Precision.HIGHEST)[0]

def reference(activations, kernel, gain, cotangent):
    weights = kernel.astype(jnp.float32)
    total = jnp.float32(PIXELS)

    def moments(pair):
        image = pair[0].astype(jnp.float32)
        grad = pair[1].astype(jnp.float32)
        pre = convolve(image, weights)
        return jnp.stack([lax.optimization_barrier(jnp.sum(pre, axis=(1, 2))), lax.optimization_barrier(jnp.sum(pre * pre, axis=(1, 2))), lax.optimization_barrier(jnp.sum(grad, axis=(1, 2))), lax.optimization_barrier(jnp.sum(grad * pre, axis=(1, 2)))])
    sums = lax.optimization_barrier(jnp.sum(lax.map(moments, (activations, cotangent)), axis=0))
    mean = sums[0] / total
    rstd = lax.rsqrt(sums[1] / total - mean * mean + 1e-05)
    sum_cot = sums[2]
    sum_norm = (sums[3] - mean * sum_cot) * rstd

    def backward(accum, pair):
        image = pair[0].astype(jnp.float32)
        grad = pair[1].astype(jnp.float32)
        pre = convolve(image, weights)
        normed = (pre - mean[:, None, None]) * rstd[:, None, None]
        pre_grad = (gain * rstd)[:, None, None] * (grad - (sum_cot / total)[:, None, None] - normed * (sum_norm / total)[:, None, None])
        pre_grad = pre_grad.astype(jnp.bfloat16).astype(jnp.float32)
        outputs, pullback = jax.vjp(convolve, image, weights)
        image_grad, weight_part = pullback(pre_grad)
        return (accum + weight_part, image_grad.astype(jnp.bfloat16))
    weight_sum, input_grad = lax.scan(backward, jnp.zeros((3, 3, C, C), jnp.float32), (activations, cotangent))
    factor = total ** (-0.5)
    return (input_grad, weight_sum * factor, sum_norm / total, sum_cot / total)
```

```python
import functools

import jax
import jax.numpy as jnp
from jax import lax
from jax.experimental import pallas as pl
from jax.experimental.pallas import tpu as pltpu
from jax.sharding import PartitionSpec as P

MESH = pl.DeviceIdType.MESH
F32 = jnp.float32
BF16 = jnp.bfloat16


def remote(src, dst, send, recv, device):
    return pltpu.make_async_remote_copy(
        src_ref=src, dst_ref=dst, send_sem=send, recv_sem=recv,
        device_id=device, device_id_type=MESH,
    )


def body(
    sizes, total,
    x_ref, cot_ref, wf_ref, wfe_ref, wb_ref, wbe_ref, gain_ref,
    out_ref, wg_ref, small_ref,
    xp, pre, x3, pgz, edge, rows_in, cols_out, cols_in, mine, grp, dps,
    acc, wdp, wpart, wgrp, wfin,
    row_s, row_r, col_s, col_r, ga_s, ga_r, gb_s, gb_r,
    wd_s, wd_r, wr_s, wr_r, wa_s, wa_r,
):
    n_dp, n_row, n_col = sizes
    n_grp = n_row * n_col
    height, channels, width = x_ref.shape
    half = width - 128
    dp, row, col = lax.axis_index("dp"), lax.axis_index("row"), lax.axis_index("col")
    me = row * n_col + col

    def member(k):
        k = lax.rem(me + k, n_grp)
        return k, (dp, k // n_col, lax.rem(k, n_col))

    def replica(k):
        k = lax.rem(dp + k, n_dp)
        return k, (k, row, col)

    barrier = pltpu.get_barrier_semaphore()
    for k in range(1, n_grp):
        pl.semaphore_signal(barrier, inc=1, device_id=member(k)[1], device_id_type=MESH)
    for k in range(1, n_dp):
        pl.semaphore_signal(barrier, inc=1, device_id=replica(k)[1], device_id_type=MESH)

    def sides(axis_pos, count, make):
        return ((axis_pos > 0, make(axis_pos - 1)), (axis_pos < count - 1, make(axis_pos + 1)))

    row_sides = sides(row, n_row, lambda r: (dp, r, col))
    col_sides = sides(col, n_col, lambda c: (dp, row, c))

    def exchange(which, near, sources, landing, send, recv):
        copies = []
        for s in range(2):
            exists, device = near[s]
            out = remote(sources[s], landing.at[which, 1 - s], send.at[which, s], recv.at[which, 1 - s], device)
            pl.when(exists)(out.start)
            copies.append(out)
        return copies

    def finish(which, near, sources, landing, send, recv):
        for s in range(2):
            exists, device = near[s]
            inc = remote(sources[s], landing.at[which, s], send.at[which, s], recv.at[which, s], device)

            @pl.when(exists)
            def _():
                inc.wait_send()
                inc.wait_recv()

    lanes = lax.broadcasted_iota(jnp.int32, (channels, 128), 1)

    def conv_row(src, w_ref, start):
        rhs = src[pl.ds(start, 3)].reshape(3 * channels, width)
        p = jnp.dot(w_ref[...], rhs, preferred_element_type=F32)
        wide = lax.broadcasted_iota(jnp.int32, (channels, width), 1)
        a = pltpu.roll(p[:channels], 1, 1)
        b = pltpu.roll(p[2 * channels :], width - 1, 1)
        a = jnp.where(wide == 0, 0.0, a)
        b = jnp.where(wide == width - 1, 0.0, b)
        return p[channels : 2 * channels] + a + b

    def columns(src, offset):
        def step(r, c):
            line = src[r + offset].astype(F32)
            last = pltpu.roll(line[:, half:], r + 1, 1)
            first = pltpu.roll(line[:, :128], 64 + r, 1)
            return jnp.where(lanes == r, last, jnp.where(lanes == 64 + r, first, c))

        return lax.fori_loop(0, height + 2, step, jnp.zeros((channels, 128), F32), unroll=2)

    def received(which):
        left = jnp.where(jnp.logical_and(lanes < 64, col > 0), cols_in[which, 0].astype(F32), 0.0)
        right = jnp.where(
            jnp.logical_and(lanes >= 64, col < n_col - 1), cols_in[which, 1].astype(F32), 0.0
        )
        return left + right

    def edge_terms(w_ref, c):
        g = jnp.dot(w_ref[...], c.astype(BF16), preferred_element_type=F32)
        left = jnp.zeros((channels, 128), F32)
        right = jnp.zeros((channels, 128), F32)
        for i in range(3):
            base = 3 * channels * i
            one, two = g[base : base + channels], g[base + 2 * channels : base + 3 * channels]
            if i:
                one, two = pltpu.roll(one, 128 - i, 1), pltpu.roll(two, 128 - i, 1)
            left, right = left + one, right + two
        return jnp.where(lanes < 64, left, right)

    def at_edges(values, r):
        left = jnp.where(lanes == 0, pltpu.roll(values, lax.rem(128 - r, 128), 1), 0.0)
        right = jnp.where(lanes == 127, pltpu.roll(values, lax.rem(191 - r, 128), 1), 0.0)
        return left, right

    def fill(h, _):
        xp[h + 1] = x_ref[h]
        return 0

    lax.fori_loop(0, height, fill, 0, unroll=4)
    zero_row = jnp.zeros((channels, width), BF16)
    for p in (0, 1, height + 2, height + 3):
        pgz[p] = zero_row

    pl.semaphore_wait(barrier, n_grp - 1 + n_dp - 1)
    x_rows = (x_ref.at[0], x_ref.at[height - 1])
    exchange(0, row_sides, x_rows, rows_in, row_s, row_r)

    def conv(h, _):
        pre[h] = conv_row(xp, wf_ref, h)
        return 0

    lax.fori_loop(1, height - 1, conv, 0, unroll=2)
    finish(0, row_sides, x_rows, rows_in, row_s, row_r)

    def place(dst, which, first, last):
        for s, p in ((0, first), (1, last)):

            @pl.when(row_sides[s][0])
            def _():
                dst[p] = rows_in[which, s]

            @pl.when(jnp.logical_not(row_sides[s][0]))
            def _():
                dst[p] = zero_row

    place(xp, 0, 0, height + 1)
    cols_out[0] = columns(xp, 0).astype(BF16)
    own_cols = (cols_out.at[0], cols_out.at[0])
    exchange(0, col_sides, own_cols, cols_in, col_s, col_r)
    conv(0, 0)
    conv(height - 1, 0)
    finish(0, col_sides, own_cols, cols_in, col_s, col_r)
    c = received(0)
    edge[0] = edge_terms(wfe_ref, c)
    edge[1] = c

    def stats(h, sums):
        left, right = at_edges(edge[0], h)
        p0 = pre[h, :, :128] + left
        pre[h, :, :128] = p0
        p1 = pre[h, :, half:] + right
        pre[h, :, half:] = p1
        g0, g1 = cot_ref[h, :, :128].astype(F32), cot_ref[h, :, half:].astype(F32)
        s0, s1, s2, s3 = sums
        return (s0 + (p0 + p1), s1 + (p0 * p0 + p1 * p1), s2 + (g0 + g1), s3 + (g0 * p0 + g1 * p1))

    empty = jnp.zeros((channels, 128), F32)
    sums = lax.fori_loop(0, height, stats, (empty, empty, empty, empty))
    mine[...] = jnp.zeros((8, 128), F32)
    for q in range(4):
        mine[q : q + 1, :channels] = jnp.sum(sums[q].T, axis=0, keepdims=True)

    def share(n, others, index, source, landing, send, recv):
        copies = []
        for k in range(1, n):
            peer, device = others(k)
            out = remote(source, landing.at[index], send.at[peer], recv.at[index], device)
            out.start()
        return copies

    def gather(n, others, index, source, landing, send, recv):
        for k in range(1, n):
            peer, device = others(k)
            inc = remote(source, landing.at[peer], send.at[peer], recv.at[peer], device)
            inc.wait_send()
            inc.wait_recv()

    share(n_grp, member, me, mine, grp, ga_s, ga_r)
    grp[me] = mine[...]

    def taps(r, _):
        line = xp[r].astype(F32)
        left, right = at_edges(edge[1], r)
        a = pltpu.roll(line, 1, 1)
        b = pltpu.roll(line, width - 1, 1)
        a0 = jnp.where(lanes == 0, left, a[:, :128])
        b1 = jnp.where(lanes == 127, right, b[:, half:])
        x3[r, :channels, :128] = a0.astype(BF16)
        x3[r, :channels, half:] = a[:, half:].astype(BF16)
        x3[r, channels : 2 * channels] = xp[r]
        x3[r, 2 * channels :, :128] = b[:, :128].astype(BF16)
        x3[r, 2 * channels :, half:] = b1.astype(BF16)
        return 0

    lax.fori_loop(0, height + 2, taps, 0, unroll=2)

    gather(n_grp, member, me, mine, grp, ga_s, ga_r)
    mine[...] = jnp.sum(grp[...], axis=0)
    share(n_dp, replica, dp, mine, dps, gb_s, gb_r)
    dps[dp] = mine[...]
    gather(n_dp, replica, dp, mine, dps, gb_s, gb_r)
    sums = jnp.sum(dps[...], axis=0)

    def derive(sum_pre, sum_sq, sum_cot, sum_cross):
        mean = sum_pre / total
        rstd = lax.rsqrt(sum_sq / total - mean * mean + 1e-05)
        sum_norm = (sum_cross - mean * sum_cot) * rstd
        return mean, rstd, sum_norm / total, sum_cot / total

    _, _, norm_row, cot_row = derive(*(sums[q : q + 1] for q in range(4)))
    small_ref[...] = jnp.concatenate([norm_row, cot_row, sums[2:]], axis=0)
    tall = [jnp.broadcast_to(sums[q : q + 1], (128, 128)).T[:channels] for q in range(4)]
    mean, rstd, norm, cmean = derive(*tall)
    scale = gain_ref[...] * rstd
    for k, v in enumerate((mean, rstd, norm, cmean, scale)):
        edge[2 + k] = v

    def grad_row(h, _):
        for a in (0, half):
            g = cot_ref[h, :, a : a + 128].astype(F32)
            normed = (pre[h, :, a : a + 128] - edge[2]) * edge[3]
            pgz[h + 2, :, a : a + 128] = (edge[6] * (g - edge[5] - normed * edge[4])).astype(BF16)
        return 0

    grad_row(0, 0)
    grad_row(height - 1, 0)
    g_rows = (pgz.at[2], pgz.at[height + 1])
    exchange(1, row_sides, g_rows, rows_in, row_s, row_r)
    lax.fori_loop(1, height - 1, grad_row, 0, unroll=2)

    acc[...] = jnp.zeros_like(acc)

    def weight(r, _):
        lhs = pgz[pl.ds(r, 3)].reshape(3 * channels, width)
        acc[...] += lax.dot_general(
            lhs, x3[r], (((1,), (1,)), ((), ())), preferred_element_type=F32
        ).reshape(acc.shape)
        return 0

    lax.fori_loop(0, height + 2, weight, 0, unroll=2)
    acc[...] = acc[...] * (total ** -0.5)
    part = channels // n_dp

    def slab(k):
        return acc.at[:, pl.ds(pl.multiple_of(k * part, 8), part), :]

    for k in range(1, n_dp):
        peer, device = replica(k)
        remote(slab(peer), wdp.at[dp], wd_s.at[peer], wd_r.at[dp], device).start()
    wdp[dp] = acc[:, pl.ds(pl.multiple_of(dp * part, 8), part), :]

    finish(1, row_sides, g_rows, rows_in, row_s, row_r)
    place(pgz, 1, 1, height + 2)
    cols_out[1] = columns(pgz, 1).astype(BF16)
    own_grads = (cols_out.at[1], cols_out.at[1])
    exchange(1, col_sides, own_grads, cols_in, col_s, col_r)

    for k in range(1, n_dp):
        peer, device = replica(k)
        inc = remote(slab(peer), wdp.at[peer], wd_s.at[peer], wd_r.at[peer], device)
        inc.wait_send()
        inc.wait_recv()
    tiles = wpart.shape[0]
    wpart[...] = jnp.sum(wdp[...], axis=0).reshape(wpart.shape)

    def owner(t):
        k = t % n_grp
        return k, (dp, k // n_col, k % n_col)

    for t in range(tiles):
        k, device = owner(t)

        @pl.when(me != k)
        def _():
            remote(wpart.at[t], wgrp.at[t // n_grp, me], wr_s.at[t], wr_r.at[t // n_grp, me], device).start()

        @pl.when(me == k)
        def _():
            wgrp[t // n_grp, me] = wpart[t]

    def back(h, _):
        pre[h] = conv_row(pgz, wb_ref, h + 1)
        return 0

    lax.fori_loop(0, height, back, 0, unroll=2)

    for t in range(tiles):
        k, device = owner(t)
        level = t // n_grp

        @pl.when(me != k)
        def _():
            remote(wpart.at[t], wgrp.at[level, me], wr_s.at[t], wr_r.at[level, me], device).wait_send()

        @pl.when(me == k)
        def _():
            for s in range(1, n_grp):
                peer, other = member(s)
                remote(wpart.at[t], wgrp.at[level, peer], wr_s.at[t], wr_r.at[level, peer], other).wait_recv()
            wfin[t] = jnp.sum(wgrp[level], axis=0)
            for s in range(1, n_grp):
                peer, other = member(s)
                remote(wfin.at[t], wfin.at[t], wa_s.at[t, peer], wa_r.at[t], other).start()

    finish(1, col_sides, own_grads, cols_in, col_s, col_r)
    edge[0] = edge_terms(wbe_ref, received(1))

    def store(h, _):
        left, right = at_edges(edge[0], h)
        out_ref[h, :, :128] = (pre[h, :, :128] + left).astype(BF16)
        out_ref[h, :, half:] = (pre[h, :, half:] + right).astype(BF16)
        return 0

    lax.fori_loop(0, height, store, 0, unroll=2)

    for t in range(tiles):
        k, device = owner(t)

        @pl.when(me == k)
        def _():
            for s in range(1, n_grp):
                peer, other = member(s)
                remote(wfin.at[t], wfin.at[t], wa_s.at[t, peer], wa_r.at[t], other).wait_send()

        @pl.when(me != k)
        def _():
            remote(wfin.at[t], wfin.at[t], wa_s.at[t, 0], wa_r.at[t], device).wait_recv()

    wg_ref[...] = wfin[...]


def per_device(sizes, activations, kernel, gain, cotangent):
    images, channels, height, width = activations.shape
    n_dp, n_row, n_col = sizes
    n_grp = n_row * n_col
    total = float(images * height * width * n_dp * n_grp)
    x = activations[0].transpose(1, 0, 2)
    cot = cotangent[0].transpose(1, 0, 2)
    wf = kernel.transpose(1, 2, 0, 3).reshape(3 * channels, 3 * channels)
    wfe = kernel.reshape(9 * channels, channels)
    flipped = kernel[::-1, ::-1].transpose(0, 1, 3, 2)
    wb = flipped.transpose(1, 2, 0, 3).reshape(3 * channels, 3 * channels)
    wbe = flipped.reshape(9 * channels, channels)
    gains = jnp.broadcast_to(gain[:, None], (channels, 128))
    part = channels // n_dp
    tiles = 3 * part // 8 if part >= 8 else 3
    tile_rows = 3 * part // tiles
    levels = -(-tiles // n_grp)
    dma = pltpu.SemaphoreType.DMA
    vmem = pl.BlockSpec(memory_space=pltpu.VMEM)
    out, wg, small = pl.pallas_call(
        functools.partial(body, sizes, total),
        out_shape=(
            jax.ShapeDtypeStruct((height, channels, width), BF16),
            jax.ShapeDtypeStruct((tiles, tile_rows, 3 * channels), F32),
            jax.ShapeDtypeStruct((8, 128), F32),
        ),
        in_specs=[vmem] * 7,
        out_specs=(vmem, vmem, vmem),
        scratch_shapes=[
            pltpu.VMEM((height + 2, channels, width), BF16),
            pltpu.VMEM((height, channels, width), F32),
            pltpu.VMEM((height + 2, 3 * channels, width), BF16),
            pltpu.VMEM((height + 4, channels, width), BF16),
            pltpu.VMEM((7, channels, 128), F32),
            pltpu.VMEM((2, 2, channels, width), BF16),
            pltpu.VMEM((2, channels, 128), BF16),
            pltpu.VMEM((2, 2, channels, 128), BF16),
            pltpu.VMEM((8, 128), F32),
            pltpu.VMEM((n_grp, 8, 128), F32),
            pltpu.VMEM((n_dp, 8, 128), F32),
            pltpu.VMEM((3, channels, 3 * channels), F32),
            pltpu.VMEM((n_dp, 3, part, 3 * channels), F32),
            pltpu.VMEM((tiles, tile_rows, 3 * channels), F32),
            pltpu.VMEM((levels, n_grp, tile_rows, 3 * channels), F32),
            pltpu.VMEM((tiles, tile_rows, 3 * channels), F32),
            dma((2, 2)), dma((2, 2)), dma((2, 2)), dma((2, 2)),
            dma((n_grp,)), dma((n_grp,)), dma((n_dp,)), dma((n_dp,)),
            dma((n_dp,)), dma((n_dp,)),
            dma((tiles,)), dma((levels, n_grp)),
            dma((tiles, n_grp)), dma((tiles,)),
        ],
        compiler_params=pltpu.CompilerParams(
            collective_id=0, has_side_effects=True, vmem_limit_bytes=40 * 1024 * 1024
        ),
    )(x, cot, wf, wfe, wb, wbe, gains)
    input_grad = out.transpose(1, 0, 2)[None]
    weight_grad = wg.reshape(3, part, 3, channels)[::-1].transpose(0, 2, 1, 3)
    return input_grad, weight_grad, small[0, :channels], small[1, :channels]


def solution(mesh):
    sizes = tuple(mesh.shape[a] for a in ("dp", "row", "col"))
    return jax.shard_map(
        functools.partial(per_device, sizes),
        mesh=mesh,
        in_specs=(P("dp", None, "row", "col"), P(), P(), P("dp", None, "row", "col")),
        out_specs=(P("dp", None, "row", "col"), P(None, None, "dp", None), P(), P()),
        check_vma=False,
    )
```

```python
import functools

import jax
import jax.numpy as jnp
from jax import lax
from jax.experimental import pallas as pl
from jax.experimental.pallas import tpu as pltpu
from jax.sharding import PartitionSpec as P

MESH = pl.DeviceIdType.MESH
F32 = jnp.float32
BF16 = jnp.bfloat16


def remote(src, dst, send, recv, device):
    return pltpu.make_async_remote_copy(
        src_ref=src, dst_ref=dst, send_sem=send, recv_sem=recv,
        device_id=device, device_id_type=MESH,
    )


def body(
    sizes, total,
    x_ref, cot_ref, wfe_ref, gain_ref,
    out_ref, wg_ref, norm_ref, shift_ref,
    wf_ref, wb_ref, wbe_ref,
    xp, pre, x3, pgz, edge, rows_in, cols_out, cols_in, mine, grp, dps,
    acc, wdp, wpart, wgrp, wfin,
    row_s, row_r, col_s, col_r, ga_s, ga_r, gb_s, gb_r,
    wd_s, wd_r, wr_s, wr_r, wa_s, wa_r,
):
    n_dp, n_row, n_col = sizes
    n_grp = n_row * n_col
    height, channels, width = x_ref.shape
    half = width - 128
    dp, row, col = lax.axis_index("dp"), lax.axis_index("row"), lax.axis_index("col")
    me = row * n_col + col

    def member(k):
        k = lax.rem(me + k, n_grp)
        return k, (dp, k // n_col, lax.rem(k, n_col))

    def replica(k):
        k = lax.rem(dp + k, n_dp)
        return k, (k, row, col)

    barrier = pltpu.get_barrier_semaphore()
    for k in range(1, n_grp):
        pl.semaphore_signal(barrier, inc=1, device_id=member(k)[1], device_id_type=MESH)
    for k in range(1, n_dp):
        pl.semaphore_signal(barrier, inc=1, device_id=replica(k)[1], device_id_type=MESH)

    def sides(axis_pos, count, make):
        return ((axis_pos > 0, make(axis_pos - 1)), (axis_pos < count - 1, make(axis_pos + 1)))

    row_sides = sides(row, n_row, lambda r: (dp, r, col))
    col_sides = sides(col, n_col, lambda c: (dp, row, c))

    def exchange(which, near, sources, landing, send, recv):
        copies = []
        for s in range(2):
            exists, device = near[s]
            out = remote(sources[s], landing.at[which, 1 - s], send.at[which, s], recv.at[which, 1 - s], device)
            pl.when(exists)(out.start)
            copies.append(out)
        return copies

    def finish(which, near, sources, landing, send, recv):
        for s in range(2):
            exists, device = near[s]
            inc = remote(sources[s], landing.at[which, s], send.at[which, s], recv.at[which, s], device)

            @pl.when(exists)
            def _():
                inc.wait_send()
                inc.wait_recv()

    lanes = lax.broadcasted_iota(jnp.int32, (channels, 128), 1)

    def conv_row(src, w_ref, start):
        rhs = src[pl.ds(start, 3)].reshape(3 * channels, width)
        p = jnp.dot(w_ref[...], rhs, preferred_element_type=F32)
        wide = lax.broadcasted_iota(jnp.int32, (channels, width), 1)
        a = pltpu.roll(p[:channels], 1, 1)
        b = pltpu.roll(p[2 * channels :], width - 1, 1)
        a = jnp.where(wide == 0, 0.0, a)
        b = jnp.where(wide == width - 1, 0.0, b)
        return p[channels : 2 * channels] + a + b

    def columns(src, offset):
        def step(r, c):
            line = src[r + offset].astype(F32)
            last = pltpu.roll(line[:, half:], r + 1, 1)
            first = pltpu.roll(line[:, :128], 64 + r, 1)
            return jnp.where(lanes == r, last, jnp.where(lanes == 64 + r, first, c))

        return lax.fori_loop(0, height + 2, step, jnp.zeros((channels, 128), F32), unroll=8)

    def received(which):
        left = jnp.where(jnp.logical_and(lanes < 64, col > 0), cols_in[which, 0].astype(F32), 0.0)
        right = jnp.where(
            jnp.logical_and(lanes >= 64, col < n_col - 1), cols_in[which, 1].astype(F32), 0.0
        )
        return left + right

    def edge_terms(w_ref, c):
        g = jnp.dot(w_ref[...], c.astype(BF16), preferred_element_type=F32)
        left = jnp.zeros((channels, 128), F32)
        right = jnp.zeros((channels, 128), F32)
        for i in range(3):
            base = 3 * channels * i
            one, two = g[base : base + channels], g[base + 2 * channels : base + 3 * channels]
            if i:
                one, two = pltpu.roll(one, 128 - i, 1), pltpu.roll(two, 128 - i, 1)
            left, right = left + one, right + two
        return jnp.where(lanes < 64, left, right)

    def at_edges(values, r):
        spots = lanes[: values.shape[0]]
        left = jnp.where(spots == 0, pltpu.roll(values, lax.rem(128 - r, 128), 1), 0.0)
        right = jnp.where(spots == 127, pltpu.roll(values, lax.rem(191 - r, 128), 1), 0.0)
        return left, right

    def fill(h, _):
        xp[h + 1] = x_ref[h]
        return 0

    lax.fori_loop(0, height, fill, 0, unroll=4)
    zero_row = jnp.zeros((channels, width), BF16)

    def tap(i, j):
        base = channels * (3 * i + j)
        return wfe_ref[base : base + channels].astype(F32)

    for j in range(3):
        rows = slice(j * channels, (j + 1) * channels)
        wf_ref[rows] = jnp.concatenate([tap(i, j) for i in range(3)], axis=1).astype(BF16)
        back_taps = [tap(2 - i, 2 - j).T for i in range(3)]
        wb_ref[rows] = jnp.concatenate(back_taps, axis=1).astype(BF16)
        for i in range(3):
            base = channels * (3 * i + j)
            wbe_ref[base : base + channels] = back_taps[i].astype(BF16)

    for p in (0, 1, height + 2, height + 3):
        pgz[p] = zero_row

    pl.semaphore_wait(barrier, n_grp - 1 + n_dp - 1)
    x_rows = (x_ref.at[0], x_ref.at[height - 1])
    exchange(0, row_sides, x_rows, rows_in, row_s, row_r)

    def conv(h, _):
        pre[h] = conv_row(xp, wf_ref, h)
        return 0

    lax.fori_loop(1, height - 1, conv, 0, unroll=6)
    finish(0, row_sides, x_rows, rows_in, row_s, row_r)

    def place(dst, which, first, last):
        for s, p in ((0, first), (1, last)):

            @pl.when(row_sides[s][0])
            def _():
                dst[p] = rows_in[which, s]

            @pl.when(jnp.logical_not(row_sides[s][0]))
            def _():
                dst[p] = zero_row

    place(xp, 0, 0, height + 1)
    cols_out[0] = columns(xp, 0).astype(BF16)
    own_cols = (cols_out.at[0], cols_out.at[0])
    exchange(0, col_sides, own_cols, cols_in, col_s, col_r)
    conv(0, 0)
    conv(height - 1, 0)
    finish(0, col_sides, own_cols, cols_in, col_s, col_r)
    c = received(0)
    edge[0] = edge_terms(wfe_ref, c)
    edge[1] = c

    def stats(part, h, sums):
        left, right = at_edges(edge[0, part], h)
        p0 = pre[h, part, :128] + left
        pre[h, part, :128] = p0
        p1 = pre[h, part, half:] + right
        pre[h, part, half:] = p1
        g0, g1 = cot_ref[h, part, :128].astype(F32), cot_ref[h, part, half:].astype(F32)
        s0, s1, s2, s3 = sums
        return (s0 + (p0 + p1), s1 + (p0 * p0 + p1 * p1), s2 + (g0 + g1), s3 + (g0 * p0 + g1 * p1))

    halves = []
    for k in range(2):
        part = slice(k * channels // 2, (k + 1) * channels // 2)
        empty = jnp.zeros((channels // 2, 128), F32)
        halves.append(
            lax.fori_loop(0, height, functools.partial(stats, part), (empty,) * 4, unroll=4)
        )
    sums = [jnp.concatenate(pair, axis=0) for pair in zip(*halves)]
    mine[...] = jnp.zeros((8, 128), F32)
    for q in range(4):
        mine[q : q + 1, :channels] = jnp.sum(sums[q].T, axis=0, keepdims=True)

    def share(n, others, index, source, landing, send, recv):
        copies = []
        for k in range(1, n):
            peer, device = others(k)
            out = remote(source, landing.at[index], send.at[peer], recv.at[index], device)
            out.start()
        return copies

    def gather(n, others, index, source, landing, send, recv):
        for k in range(1, n):
            peer, device = others(k)
            inc = remote(source, landing.at[peer], send.at[peer], recv.at[peer], device)
            inc.wait_send()
            inc.wait_recv()

    share(n_grp, member, me, mine, grp, ga_s, ga_r)
    grp[me] = mine[...]

    def taps(r, _):
        line = xp[r].astype(F32)
        left, right = at_edges(edge[1], r)
        a = pltpu.roll(line, 1, 1)
        b = pltpu.roll(line, width - 1, 1)
        a0 = jnp.where(lanes == 0, left, a[:, :128])
        b1 = jnp.where(lanes == 127, right, b[:, half:])
        x3[r, :channels, :128] = a0.astype(BF16)
        x3[r, :channels, half:] = a[:, half:].astype(BF16)
        x3[r, channels : 2 * channels] = xp[r]
        x3[r, 2 * channels :, :128] = b[:, :128].astype(BF16)
        x3[r, 2 * channels :, half:] = b1.astype(BF16)
        return 0

    lax.fori_loop(0, height + 2, taps, 0, unroll=4)

    gather(n_grp, member, me, mine, grp, ga_s, ga_r)
    mine[...] = jnp.sum(grp[...], axis=0)
    share(n_dp, replica, dp, mine, dps, gb_s, gb_r)
    dps[dp] = mine[...]
    gather(n_dp, replica, dp, mine, dps, gb_s, gb_r)
    sums = jnp.sum(dps[...], axis=0)

    def derive(sum_pre, sum_sq, sum_cot, sum_cross):
        mean = sum_pre / total
        rstd = lax.rsqrt(sum_sq / total - mean * mean + 1e-05)
        sum_norm = (sum_cross - mean * sum_cot) * rstd
        return mean, rstd, sum_norm / total, sum_cot / total

    _, _, norm_row, cot_row = derive(*(sums[q : q + 1] for q in range(4)))
    norm_ref[...] = norm_row[:, :channels]
    shift_ref[...] = cot_row[:, :channels]
    tall = [jnp.broadcast_to(sums[q : q + 1], (128, 128)).T[:channels] for q in range(4)]
    mean, rstd, norm, cmean = derive(*tall)
    scale = jnp.broadcast_to(gain_ref[...], (128, channels)).T * rstd
    for k, v in enumerate((mean, rstd, norm, cmean, scale)):
        edge[2 + k] = v

    def grad_row(h, _):
        for a in (0, half):
            g = cot_ref[h, :, a : a + 128].astype(F32)
            normed = (pre[h, :, a : a + 128] - edge[2]) * edge[3]
            pgz[h + 2, :, a : a + 128] = (edge[6] * (g - edge[5] - normed * edge[4])).astype(BF16)
        return 0

    grad_row(0, 0)
    grad_row(height - 1, 0)
    g_rows = (pgz.at[2], pgz.at[height + 1])
    exchange(1, row_sides, g_rows, rows_in, row_s, row_r)
    lax.fori_loop(1, height - 1, grad_row, 0, unroll=2)

    acc[...] = jnp.zeros_like(acc)

    def weight(rows, r):
        lhs = [pgz[pl.ds(r + k, 3)].reshape(3 * channels, width) for k in range(rows)]
        rhs = [x3[r + k] for k in range(rows)]
        acc[...] += lax.dot_general(
            jnp.concatenate(lhs, axis=1), jnp.concatenate(rhs, axis=1),
            (((1,), (1,)), ((), ())), preferred_element_type=F32,
        ).reshape(acc.shape)

    whole = (height + 2) // 8

    def weights(k, _):
        weight(8, k * 8)
        return 0

    lax.fori_loop(0, whole, weights, 0)
    if (height + 2) % 8:
        weight((height + 2) % 8, whole * 8)
    acc[...] = acc[...] * (total ** -0.5)
    part = channels // n_dp

    def slab(k):
        return acc.at[:, pl.ds(pl.multiple_of(k * part, 8), part), :]

    for k in range(1, n_dp):
        peer, device = replica(k)
        remote(slab(peer), wdp.at[dp], wd_s.at[peer], wd_r.at[dp], device).start()
    wdp[dp] = acc[:, pl.ds(pl.multiple_of(dp * part, 8), part), :]

    finish(1, row_sides, g_rows, rows_in, row_s, row_r)
    place(pgz, 1, 1, height + 2)
    cols_out[1] = columns(pgz, 1).astype(BF16)
    own_grads = (cols_out.at[1], cols_out.at[1])
    exchange(1, col_sides, own_grads, cols_in, col_s, col_r)

    for k in range(1, n_dp):
        peer, device = replica(k)
        inc = remote(slab(peer), wdp.at[peer], wd_s.at[peer], wd_r.at[peer], device)
        inc.wait_send()
        inc.wait_recv()
    tiles = wpart.shape[0]
    wpart[...] = jnp.sum(wdp[...], axis=0).reshape(wpart.shape)

    def owner(t):
        k = t % n_grp
        return k, (dp, k // n_col, k % n_col)

    for t in range(tiles):
        k, device = owner(t)

        @pl.when(me != k)
        def _():
            remote(wpart.at[t], wgrp.at[t // n_grp, me], wr_s.at[t], wr_r.at[t // n_grp, me], device).start()

        @pl.when(me == k)
        def _():
            wgrp[t // n_grp, me] = wpart[t]

    def back(h, _):
        pre[h] = conv_row(pgz, wb_ref, h + 1)
        return 0

    lax.fori_loop(0, height, back, 0, unroll=8)

    for t in range(tiles):
        k, device = owner(t)
        level = t // n_grp

        @pl.when(me != k)
        def _():
            remote(wpart.at[t], wgrp.at[level, me], wr_s.at[t], wr_r.at[level, me], device).wait_send()

        @pl.when(me == k)
        def _():
            for s in range(1, n_grp):
                peer, other = member(s)
                remote(wpart.at[t], wgrp.at[level, peer], wr_s.at[t], wr_r.at[level, peer], other).wait_recv()
            wfin[t] = jnp.sum(wgrp[level], axis=0)
            for s in range(1, n_grp):
                peer, other = member(s)
                remote(wfin.at[t], wfin.at[t], wa_s.at[t, peer], wa_r.at[t], other).start()

    finish(1, col_sides, own_grads, cols_in, col_s, col_r)
    edge[0] = edge_terms(wbe_ref, received(1))

    def store(h, _):
        left, right = at_edges(edge[0], h)
        out_ref[h, :, :128] = (pre[h, :, :128] + left).astype(BF16)
        out_ref[h, :, half:] = (pre[h, :, half:] + right).astype(BF16)
        return 0

    lax.fori_loop(0, height, store, 0, unroll=8)

    for t in range(tiles):
        k, device = owner(t)

        @pl.when(me == k)
        def _():
            for s in range(1, n_grp):
                peer, other = member(s)
                remote(wfin.at[t], wfin.at[t], wa_s.at[t, peer], wa_r.at[t], other).wait_send()

        @pl.when(me != k)
        def _():
            remote(wfin.at[t], wfin.at[t], wa_s.at[t, 0], wa_r.at[t], device).wait_recv()

    tile_rows = wfin.shape[1]
    for t in range(tiles):
        a, o = divmod(t * tile_rows, channels // n_dp)
        for j in range(3):
            wg_ref[2 - a, j, o : o + tile_rows] = wfin[t, :, j * channels : (j + 1) * channels]


def per_device(sizes, activations, kernel, gain, cotangent):
    images, channels, height, width = activations.shape
    n_dp, n_row, n_col = sizes
    n_grp = n_row * n_col
    total = float(images * height * width * n_dp * n_grp)
    x = activations[0].transpose(1, 0, 2)
    cot = cotangent[0].transpose(1, 0, 2)
    taps = kernel.reshape(9 * channels, channels)
    part = channels // n_dp
    tiles = 3 * part // 8 if part >= 8 else 3
    tile_rows = 3 * part // tiles
    levels = -(-tiles // n_grp)
    dma = pltpu.SemaphoreType.DMA
    vmem = pl.BlockSpec(memory_space=pltpu.VMEM)
    out, weight_grad, norm, shift = pl.pallas_call(
        functools.partial(body, sizes, total),
        out_shape=(
            jax.ShapeDtypeStruct((height, channels, width), BF16),
            jax.ShapeDtypeStruct((3, 3, part, channels), F32),
            jax.ShapeDtypeStruct((1, channels), F32),
            jax.ShapeDtypeStruct((1, channels), F32),
        ),
        in_specs=[vmem] * 4,
        out_specs=(vmem,) * 4,
        scratch_shapes=[
            pltpu.VMEM((3 * channels, 3 * channels), BF16),
            pltpu.VMEM((3 * channels, 3 * channels), BF16),
            pltpu.VMEM((9 * channels, channels), BF16),
            pltpu.VMEM((height + 2, channels, width), BF16),
            pltpu.VMEM((height, channels, width), F32),
            pltpu.VMEM((height + 2, 3 * channels, width), BF16),
            pltpu.VMEM((height + 4, channels, width), BF16),
            pltpu.VMEM((7, channels, 128), F32),
            pltpu.VMEM((2, 2, channels, width), BF16),
            pltpu.VMEM((2, channels, 128), BF16),
            pltpu.VMEM((2, 2, channels, 128), BF16),
            pltpu.VMEM((8, 128), F32),
            pltpu.VMEM((n_grp, 8, 128), F32),
            pltpu.VMEM((n_dp, 8, 128), F32),
            pltpu.VMEM((3, channels, 3 * channels), F32),
            pltpu.VMEM((n_dp, 3, part, 3 * channels), F32),
            pltpu.VMEM((tiles, tile_rows, 3 * channels), F32),
            pltpu.VMEM((levels, n_grp, tile_rows, 3 * channels), F32),
            pltpu.VMEM((tiles, tile_rows, 3 * channels), F32),
            dma((2, 2)), dma((2, 2)), dma((2, 2)), dma((2, 2)),
            dma((n_grp,)), dma((n_grp,)), dma((n_dp,)), dma((n_dp,)),
            dma((n_dp,)), dma((n_dp,)),
            dma((tiles,)), dma((levels, n_grp)),
            dma((tiles, n_grp)), dma((tiles,)),
        ],
        compiler_params=pltpu.CompilerParams(
            collective_id=0, has_side_effects=True, vmem_limit_bytes=40 * 1024 * 1024
        ),
    )(x, cot, taps, gain[None])
    input_grad = out.transpose(1, 0, 2)[None]
    return input_grad, weight_grad, norm[0], shift[0]


def solution(mesh):
    sizes = tuple(mesh.shape[a] for a in ("dp", "row", "col"))
    return jax.shard_map(
        functools.partial(per_device, sizes),
        mesh=mesh,
        in_specs=(P("dp", None, "row", "col"), P(), P(), P("dp", None, "row", "col")),
        out_specs=(P("dp", None, "row", "col"), P(None, None, "dp", None), P(), P()),
        check_vma=False,
    )
```

```python
import functools

import jax
import jax.numpy as jnp
from jax import lax
from jax.experimental import pallas as pl
from jax.experimental.pallas import tpu as pltpu
from jax.sharding import PartitionSpec as P

MESH = pl.DeviceIdType.MESH
F32 = jnp.float32
BF16 = jnp.bfloat16


def remote(src, dst, send, recv, device):
    return pltpu.make_async_remote_copy(
        src_ref=src, dst_ref=dst, send_sem=send, recv_sem=recv,
        device_id=device, device_id_type=MESH,
    )


def body(
    sizes, total,
    x_ref, cot_ref, taps_ref, gains_ref,
    out_ref, wg_ref, small_ref,
    wfe_ref, gain_ref, own_s,
    wf_ref, wb_ref, wbe_ref,
    xp, pre, x3, pgz, edge, rows_in, cols_out, cols_in, mine, grp, dps,
    acc, wdp, wpart, wgrp, wfin,
    row_s, row_r, col_s, col_r, ga_s, ga_r, gb_s, gb_r,
    wd_s, wd_r, wr_s, wr_r, wa_s, wa_r,
):
    n_dp, n_row, n_col = sizes
    n_grp = n_row * n_col
    height, channels, width = x_ref.shape
    half = width - 128
    dp, row, col = lax.axis_index("dp"), lax.axis_index("row"), lax.axis_index("col")
    me = row * n_col + col

    def member(k):
        k = lax.rem(me + k, n_grp)
        return k, (dp, k // n_col, lax.rem(k, n_col))

    def replica(k):
        k = lax.rem(dp + k, n_dp)
        return k, (k, row, col)

    fetch_taps = pltpu.make_async_copy(taps_ref, wfe_ref, own_s.at[0])
    fetch_gain = pltpu.make_async_copy(gains_ref, gain_ref, own_s.at[1])
    fetch_taps.start()
    fetch_gain.start()
    barrier = pltpu.get_barrier_semaphore()
    for k in range(1, n_grp):
        pl.semaphore_signal(barrier, inc=1, device_id=member(k)[1], device_id_type=MESH)
    for k in range(1, n_dp):
        pl.semaphore_signal(barrier, inc=1, device_id=replica(k)[1], device_id_type=MESH)

    def sides(axis_pos, count, make):
        return ((axis_pos > 0, make(axis_pos - 1)), (axis_pos < count - 1, make(axis_pos + 1)))

    row_sides = sides(row, n_row, lambda r: (dp, r, col))
    col_sides = sides(col, n_col, lambda c: (dp, row, c))

    def exchange(which, near, sources, landing, send, recv):
        copies = []
        for s in range(2):
            exists, device = near[s]
            out = remote(sources[s], landing.at[which, 1 - s], send.at[which, s], recv.at[which, 1 - s], device)
            pl.when(exists)(out.start)
            copies.append(out)
        return copies

    def finish(which, near, sources, landing, send, recv):
        for s in range(2):
            exists, device = near[s]
            inc = remote(sources[s], landing.at[which, s], send.at[which, s], recv.at[which, s], device)

            @pl.when(exists)
            def _():
                inc.wait_send()
                inc.wait_recv()

    lanes = lax.broadcasted_iota(jnp.int32, (channels, 128), 1)

    def conv_row(src, w_ref, start):
        rhs = src[pl.ds(start, 3)].reshape(3 * channels, width)
        p = jnp.dot(w_ref[...], rhs, preferred_element_type=F32)
        wide = lax.broadcasted_iota(jnp.int32, (channels, width), 1)
        a = pltpu.roll(p[:channels], 1, 1)
        b = pltpu.roll(p[2 * channels :], width - 1, 1)
        a = jnp.where(wide == 0, 0.0, a)
        b = jnp.where(wide == width - 1, 0.0, b)
        return p[channels : 2 * channels] + a + b

    def columns(src, offset):
        def step(r, c):
            line = src[r + offset].astype(F32)
            last = pltpu.roll(line[:, half:], r + 1, 1)
            first = pltpu.roll(line[:, :128], 64 + r, 1)
            return jnp.where(lanes == r, last, jnp.where(lanes == 64 + r, first, c))

        return lax.fori_loop(0, height + 2, step, jnp.zeros((channels, 128), F32), unroll=8)

    def received(which):
        left = jnp.where(jnp.logical_and(lanes < 64, col > 0), cols_in[which, 0].astype(F32), 0.0)
        right = jnp.where(
            jnp.logical_and(lanes >= 64, col < n_col - 1), cols_in[which, 1].astype(F32), 0.0
        )
        return left + right

    def edge_terms(w_ref, c):
        g = jnp.dot(w_ref[...], c.astype(BF16), preferred_element_type=F32)
        left = jnp.zeros((channels, 128), F32)
        right = jnp.zeros((channels, 128), F32)
        for i in range(3):
            base = 3 * channels * i
            one, two = g[base : base + channels], g[base + 2 * channels : base + 3 * channels]
            if i:
                one, two = pltpu.roll(one, 128 - i, 1), pltpu.roll(two, 128 - i, 1)
            left, right = left + one, right + two
        return jnp.where(lanes < 64, left, right)

    def at_edges(values, r):
        spots = lanes[: values.shape[0]]
        left = jnp.where(spots == 0, pltpu.roll(values, lax.rem(128 - r, 128), 1), 0.0)
        right = jnp.where(spots == 127, pltpu.roll(values, lax.rem(191 - r, 128), 1), 0.0)
        return left, right

    def fill(h, _):
        xp[h + 1] = x_ref[h]
        return 0

    lax.fori_loop(0, height, fill, 0, unroll=4)
    zero_row = jnp.zeros((channels, width), BF16)

    def tap(i, j):
        base = channels * (3 * i + j)
        return wfe_ref[base : base + channels].astype(F32)

    fetch_taps.wait()
    fetch_gain.wait()
    for j in range(3):
        rows = slice(j * channels, (j + 1) * channels)
        wf_ref[rows] = jnp.concatenate([tap(i, j) for i in range(3)], axis=1).astype(BF16)
        back_taps = [tap(2 - i, 2 - j).T for i in range(3)]
        wb_ref[rows] = jnp.concatenate(back_taps, axis=1).astype(BF16)
        for i in range(3):
            base = channels * (3 * i + j)
            wbe_ref[base : base + channels] = back_taps[i].astype(BF16)

    for p in (0, 1, height + 2, height + 3):
        pgz[p] = zero_row

    pl.semaphore_wait(barrier, n_grp - 1 + n_dp - 1)
    x_rows = (x_ref.at[0], x_ref.at[height - 1])
    exchange(0, row_sides, x_rows, rows_in, row_s, row_r)

    def conv(h, _):
        pre[h] = conv_row(xp, wf_ref, h)
        return 0

    lax.fori_loop(1, height - 1, conv, 0, unroll=10)
    finish(0, row_sides, x_rows, rows_in, row_s, row_r)

    def place(dst, which, first, last):
        for s, p in ((0, first), (1, last)):

            @pl.when(row_sides[s][0])
            def _():
                dst[p] = rows_in[which, s]

            @pl.when(jnp.logical_not(row_sides[s][0]))
            def _():
                dst[p] = zero_row

    place(xp, 0, 0, height + 1)
    cols_out[0] = columns(xp, 0).astype(BF16)
    own_cols = (cols_out.at[0], cols_out.at[0])
    exchange(0, col_sides, own_cols, cols_in, col_s, col_r)
    conv(0, 0)
    conv(height - 1, 0)
    finish(0, col_sides, own_cols, cols_in, col_s, col_r)
    c = received(0)
    edge[0] = edge_terms(wfe_ref, c)
    edge[1] = c

    def stats(part, h, sums):
        left, right = at_edges(edge[0, part], h)
        p0 = pre[h, part, :128] + left
        pre[h, part, :128] = p0
        p1 = pre[h, part, half:] + right
        pre[h, part, half:] = p1
        g0, g1 = cot_ref[h, part, :128].astype(F32), cot_ref[h, part, half:].astype(F32)
        s0, s1, s2, s3 = sums
        return (s0 + (p0 + p1), s1 + (p0 * p0 + p1 * p1), s2 + (g0 + g1), s3 + (g0 * p0 + g1 * p1))

    halves = []
    for k in range(2):
        part = slice(k * channels // 2, (k + 1) * channels // 2)
        empty = jnp.zeros((channels // 2, 128), F32)
        halves.append(
            lax.fori_loop(0, height, functools.partial(stats, part), (empty,) * 4, unroll=8)
        )
    sums = [jnp.concatenate(pair, axis=0) for pair in zip(*halves)]
    mine[...] = jnp.zeros((8, 128), F32)
    for q in range(4):
        mine[q : q + 1, :channels] = jnp.sum(sums[q].T, axis=0, keepdims=True)

    def share(n, others, index, source, landing, send, recv):
        copies = []
        for k in range(1, n):
            peer, device = others(k)
            out = remote(source, landing.at[index], send.at[peer], recv.at[index], device)
            out.start()
        return copies

    def gather(n, others, index, source, landing, send, recv):
        for k in range(1, n):
            peer, device = others(k)
            inc = remote(source, landing.at[peer], send.at[peer], recv.at[peer], device)
            inc.wait_send()
            inc.wait_recv()

    share(n_grp, member, me, mine, grp, ga_s, ga_r)
    grp[me] = mine[...]

    def taps(r, _):
        line = xp[r].astype(F32)
        left, right = at_edges(edge[1], r)
        a = pltpu.roll(line, 1, 1)
        b = pltpu.roll(line, width - 1, 1)
        a0 = jnp.where(lanes == 0, left, a[:, :128])
        b1 = jnp.where(lanes == 127, right, b[:, half:])
        x3[r, :channels, :128] = a0.astype(BF16)
        x3[r, :channels, half:] = a[:, half:].astype(BF16)
        x3[r, channels : 2 * channels] = xp[r]
        x3[r, 2 * channels :, :128] = b[:, :128].astype(BF16)
        x3[r, 2 * channels :, half:] = b1.astype(BF16)
        return 0

    lax.fori_loop(0, height + 2, taps, 0, unroll=4)

    gather(n_grp, member, me, mine, grp, ga_s, ga_r)
    mine[...] = jnp.sum(grp[...], axis=0)
    share(n_dp, replica, dp, mine, dps, gb_s, gb_r)
    dps[dp] = mine[...]
    gather(n_dp, replica, dp, mine, dps, gb_s, gb_r)
    sums = jnp.sum(dps[...], axis=0)

    def derive(sum_pre, sum_sq, sum_cot, sum_cross):
        mean = sum_pre / total
        rstd = lax.rsqrt(sum_sq / total - mean * mean + 1e-05)
        sum_norm = (sum_cross - mean * sum_cot) * rstd
        return mean, rstd, sum_norm / total, sum_cot / total

    _, _, norm_row, cot_row = derive(*(sums[q : q + 1] for q in range(4)))
    small_ref[...] = jnp.concatenate([norm_row, cot_row, sums[2:]], axis=0)
    tall = [jnp.broadcast_to(sums[q : q + 1], (128, 128)).T[:channels] for q in range(4)]
    mean, rstd, norm, cmean = derive(*tall)
    scale = jnp.broadcast_to(gain_ref[...], (128, channels)).T * rstd
    for k, v in enumerate((mean, rstd, norm, cmean, scale)):
        edge[2 + k] = v

    def grad_row(h, _):
        for a in (0, half):
            g = cot_ref[h, :, a : a + 128].astype(F32)
            normed = (pre[h, :, a : a + 128] - edge[2]) * edge[3]
            pgz[h + 2, :, a : a + 128] = (edge[6] * (g - edge[5] - normed * edge[4])).astype(BF16)
        return 0

    grad_row(0, 0)
    grad_row(height - 1, 0)
    g_rows = (pgz.at[2], pgz.at[height + 1])
    exchange(1, row_sides, g_rows, rows_in, row_s, row_r)
    lax.fori_loop(1, height - 1, grad_row, 0, unroll=6)

    acc[...] = jnp.zeros_like(acc)

    def weight(rows, r):
        lhs = [pgz[pl.ds(r + k, 3)].reshape(3 * channels, width) for k in range(rows)]
        rhs = [x3[r + k] for k in range(rows)]
        acc[...] += lax.dot_general(
            jnp.concatenate(lhs, axis=1), jnp.concatenate(rhs, axis=1),
            (((1,), (1,)), ((), ())), preferred_element_type=F32,
        ).reshape(acc.shape)

    whole = (height + 2) // 8

    def weights(k, _):
        weight(8, k * 8)
        return 0

    lax.fori_loop(0, whole, weights, 0)
    if (height + 2) % 8:
        weight((height + 2) % 8, whole * 8)
    acc[...] = acc[...] * (total ** -0.5)
    part = channels // n_dp

    def slab(k):
        return acc.at[:, pl.ds(pl.multiple_of(k * part, 8), part), :]

    for k in range(1, n_dp):
        peer, device = replica(k)
        remote(slab(peer), wdp.at[dp], wd_s.at[peer], wd_r.at[dp], device).start()
    wdp[dp] = acc[:, pl.ds(pl.multiple_of(dp * part, 8), part), :]

    finish(1, row_sides, g_rows, rows_in, row_s, row_r)
    place(pgz, 1, 1, height + 2)
    cols_out[1] = columns(pgz, 1).astype(BF16)
    own_grads = (cols_out.at[1], cols_out.at[1])
    exchange(1, col_sides, own_grads, cols_in, col_s, col_r)

    for k in range(1, n_dp):
        peer, device = replica(k)
        inc = remote(slab(peer), wdp.at[peer], wd_s.at[peer], wd_r.at[peer], device)
        inc.wait_send()
        inc.wait_recv()
    tiles = wpart.shape[0]
    wpart[...] = jnp.sum(wdp[...], axis=0).reshape(wpart.shape)

    def owner(t):
        k = t % n_grp
        return k, (dp, k // n_col, k % n_col)

    for t in range(tiles):
        k, device = owner(t)

        @pl.when(me != k)
        def _():
            remote(wpart.at[t], wgrp.at[t // n_grp, me], wr_s.at[t], wr_r.at[t // n_grp, me], device).start()

        @pl.when(me == k)
        def _():
            wgrp[t // n_grp, me] = wpart[t]

    def back(h, _):
        pre[h] = conv_row(pgz, wb_ref, h + 1)
        return 0

    lax.fori_loop(0, height, back, 0, unroll=16)

    for t in range(tiles):
        k, device = owner(t)
        level = t // n_grp

        @pl.when(me != k)
        def _():
            remote(wpart.at[t], wgrp.at[level, me], wr_s.at[t], wr_r.at[level, me], device).wait_send()

        @pl.when(me == k)
        def _():
            for s in range(1, n_grp):
                peer, other = member(s)
                remote(wpart.at[t], wgrp.at[level, peer], wr_s.at[t], wr_r.at[level, peer], other).wait_recv()
            wfin[t] = jnp.sum(wgrp[level], axis=0)
            for s in range(1, n_grp):
                peer, other = member(s)
                remote(wfin.at[t], wfin.at[t], wa_s.at[t, peer], wa_r.at[t], other).start()

    finish(1, col_sides, own_grads, cols_in, col_s, col_r)
    edge[0] = edge_terms(wbe_ref, received(1))

    def store(h, _):
        left, right = at_edges(edge[0], h)
        out_ref[h, :, :128] = (pre[h, :, :128] + left).astype(BF16)
        out_ref[h, :, half:] = (pre[h, :, half:] + right).astype(BF16)
        return 0

    lax.fori_loop(0, height, store, 0, unroll=8)

    for t in range(tiles):
        k, device = owner(t)

        @pl.when(me == k)
        def _():
            for s in range(1, n_grp):
                peer, other = member(s)
                remote(wfin.at[t], wfin.at[t], wa_s.at[t, peer], wa_r.at[t], other).wait_send()

        @pl.when(me != k)
        def _():
            remote(wfin.at[t], wfin.at[t], wa_s.at[t, 0], wa_r.at[t], device).wait_recv()

    tile_rows = wfin.shape[1]
    for t in range(tiles):
        a, o = divmod(t * tile_rows, channels // n_dp)
        for j in range(3):
            wg_ref[2 - a, j, o : o + tile_rows] = wfin[t, :, j * channels : (j + 1) * channels]


def per_device(sizes, activations, kernel, gain, cotangent):
    images, channels, height, width = activations.shape
    n_dp, n_row, n_col = sizes
    n_grp = n_row * n_col
    total = float(images * height * width * n_dp * n_grp)
    x = activations[0].transpose(1, 0, 2)
    cot = cotangent[0].transpose(1, 0, 2)
    taps = kernel.reshape(9 * channels, channels)
    part = channels // n_dp
    tiles = 3 * part // 8 if part >= 8 else 3
    tile_rows = 3 * part // tiles
    levels = -(-tiles // n_grp)
    dma = pltpu.SemaphoreType.DMA
    vmem = pl.BlockSpec(memory_space=pltpu.VMEM)
    out, weight_grad, small = pl.pallas_call(
        functools.partial(body, sizes, total),
        out_shape=(
            jax.ShapeDtypeStruct((height, channels, width), BF16),
            jax.ShapeDtypeStruct((3, 3, part, channels), F32),
            jax.ShapeDtypeStruct((8, 128), F32),
        ),
        in_specs=[vmem] * 2 + [pl.BlockSpec(memory_space=pl.ANY)] * 2,
        out_specs=(vmem,) * 3,
        scratch_shapes=[
            pltpu.VMEM((9 * channels, channels), BF16),
            pltpu.VMEM((1, channels), F32),
            dma((2,)),
            pltpu.VMEM((3 * channels, 3 * channels), BF16),
            pltpu.VMEM((3 * channels, 3 * channels), BF16),
            pltpu.VMEM((9 * channels, channels), BF16),
            pltpu.VMEM((height + 2, channels, width), BF16),
            pltpu.VMEM((height, channels, width), F32),
            pltpu.VMEM((height + 2, 3 * channels, width), BF16),
            pltpu.VMEM((height + 4, channels, width), BF16),
            pltpu.VMEM((7, channels, 128), F32),
            pltpu.VMEM((2, 2, channels, width), BF16),
            pltpu.VMEM((2, channels, 128), BF16),
            pltpu.VMEM((2, 2, channels, 128), BF16),
            pltpu.VMEM((8, 128), F32),
            pltpu.VMEM((n_grp, 8, 128), F32),
            pltpu.VMEM((n_dp, 8, 128), F32),
            pltpu.VMEM((3, channels, 3 * channels), F32),
            pltpu.VMEM((n_dp, 3, part, 3 * channels), F32),
            pltpu.VMEM((tiles, tile_rows, 3 * channels), F32),
            pltpu.VMEM((levels, n_grp, tile_rows, 3 * channels), F32),
            pltpu.VMEM((tiles, tile_rows, 3 * channels), F32),
            dma((2, 2)), dma((2, 2)), dma((2, 2)), dma((2, 2)),
            dma((n_grp,)), dma((n_grp,)), dma((n_dp,)), dma((n_dp,)),
            dma((n_dp,)), dma((n_dp,)),
            dma((tiles,)), dma((levels, n_grp)),
            dma((tiles, n_grp)), dma((tiles,)),
        ],
        compiler_params=pltpu.CompilerParams(
            collective_id=0, has_side_effects=True, vmem_limit_bytes=40 * 1024 * 1024
        ),
    )(x, cot, taps, gain[None])
    input_grad = out.transpose(1, 0, 2)[None]
    return input_grad, weight_grad, small[0, :channels], small[1, :channels]


def solution(mesh):
    sizes = tuple(mesh.shape[a] for a in ("dp", "row", "col"))
    return jax.shard_map(
        functools.partial(per_device, sizes),
        mesh=mesh,
        in_specs=(P("dp", None, "row", "col"), P(), P(), P("dp", None, "row", "col")),
        out_specs=(P("dp", None, "row", "col"), P(None, None, "dp", None), P(), P()),
        check_vma=False,
    )
```
